32 devices in a mesh: data: 32 (over z, y, x, core).
Axes of the slice: x: 2, y: 2, z: 4, core: 2. Of those that a mesh axis runs over, the one named last changes fastest.
Arguments:
- tokens: bfloat16 [32768, 1280], P('data')
- targets: bfloat16 [32768, 1280], P('data')
- w_in: bfloat16 [2, 1280, 5120], replicated
- w_out: bfloat16 [2, 5120, 1280], replicated
Outputs:
- output 1: float32 [2, 1280, 5120], P(None, 'data')
- output 2: float32 [2, 5120, 1280], P(None, 'data')
All inputs are finite; a program needn't handle non-finite values.
Results may differ from the reference program's by a relative error of at most 0.00409974.
Values are sent between devices in bfloat16 or wider.
A program may use at most 1 GiB of HBM per device.

```python
import jax
import jax.numpy as jnp
from jax import lax

D = 1280
FF = 5120
LAYERS = 2
TOKENS_DEV = 1024
DATA = 32
TOKENS = TOKENS_DEV * DATA


def setup_inputs(seed: int = 0) -> dict:
    key_root = jax.random.key(seed)
    key_tok, key_tgt, key_in, key_out = jax.random.split(key_root, 4)
    tokens = jax.random.normal(key_tok, (TOKENS, D), jnp.float32).astype(jnp.bfloat16)
    targets = (2.0 * jax.random.normal(key_tgt, (TOKENS, D), jnp.float32)).astype(jnp.bfloat16)
    w_in = (jax.random.normal(key_in, (LAYERS, D, FF), jnp.float32) * (D ** -0.5)).astype(jnp.bfloat16)
    w_out = (jax.random.normal(key_out, (LAYERS, FF, D), jnp.float32) * (0.5 * FF ** -0.5)).astype(jnp.bfloat16)
    return {"tokens": tokens, "targets": targets, "w_in": w_in, "w_out": w_out}


def gelu_act(pre_f32):
    return jax.nn.gelu(pre_f32, approximate=True)


def layer_forward(hidden, weights):
    w_first, w_second = weights
    pre_act = jnp.dot(hidden, w_first, preferred_element_type=jnp.float32).astype(jnp.bfloat16)
    act_out = gelu_act(pre_act.astype(jnp.float32)).astype(jnp.bfloat16)
    branch = jnp.dot(act_out, w_second, preferred_element_type=jnp.float32)
    new_hidden = (hidden.astype(jnp.float32) + branch).astype(jnp.bfloat16)
    return new_hidden, (hidden, pre_act, act_out)


def layer_backward(grad_h, saved_items):
    hidden, pre_act, act_out, w_first, w_second = saved_items
    grad_second = jnp.dot(act_out.T, grad_h, preferred_element_type=jnp.float32)
    grad_act = jnp.dot(grad_h, w_second.T, preferred_element_type=jnp.float32).astype(jnp.bfloat16)
    _, pullback = jax.vjp(gelu_act, pre_act.astype(jnp.float32))
    grad_pre = pullback(grad_act.astype(jnp.float32))[0].astype(jnp.bfloat16)
    grad_first = jnp.dot(hidden.T, grad_pre, preferred_element_type=jnp.float32)
    grad_below = jnp.dot(grad_pre, w_first.T, preferred_element_type=jnp.float32)
    new_grad = (grad_h.astype(jnp.float32) + grad_below).astype(jnp.bfloat16)
    return new_grad, (grad_first, grad_second)


def block_grads(tok_rows, tgt_rows, w_in, w_out):
    top_hidden, saved_fwd = lax.scan(layer_forward, tok_rows, (w_in, w_out))
    grad_top = ((top_hidden.astype(jnp.float32) - tgt_rows.astype(jnp.float32)) * (TOKENS ** -0.5)).astype(jnp.bfloat16)
    _, layer_grads = lax.scan(layer_backward, grad_top, (saved_fwd[0], saved_fwd[1], saved_fwd[2], w_in, w_out), reverse=True)
    return layer_grads


def reference(tokens, targets, w_in, w_out):
    tok_blocks = tokens.reshape(DATA, TOKENS_DEV, D)
    tgt_blocks = targets.reshape(DATA, TOKENS_DEV, D)

    def accumulate(carry, row_pair):
        grad_first, grad_second = block_grads(row_pair[0], row_pair[1], w_in, w_out)
        return (carry[0] + grad_first, carry[1] + grad_second), None

    zero_sums = (jnp.zeros((LAYERS, D, FF), jnp.float32), jnp.zeros((LAYERS, FF, D), jnp.float32))
    (sum_first, sum_second), _ = lax.scan(accumulate, zero_sums, (tok_blocks, tgt_blocks))
    return sum_first, sum_second
```

```python
import jax
import jax.numpy as jnp
from jax import lax
from jax.sharding import PartitionSpec as P


CORE, X, Y, ZL, ZH = 1, 2, 4, 8, 16
F32, BF16 = jnp.float32, jnp.bfloat16


def gelu_act(pre_f32):
    return jax.nn.gelu(pre_f32, approximate=True)


def dot(a, b, dims):
    return lax.dot_general(a, b, (dims, ((), ())), preferred_element_type=F32)


def solution(mesh):
    n = mesh.shape["data"]

    def swap(v, bit):
        return lax.ppermute(v, "data", [(i, i ^ bit) for i in range(n)])

    def local_grads(tokens, targets, w_in, w_out):
        rows, d = tokens.shape
        ff = w_in.shape[2]
        dr, fr = d // n, ff // n
        scale = (rows * n) ** -0.5
        idx = lax.axis_index("data")

        def bit(b):
            return (idx // b) % 2

        z = idx // 8

        def plane_gather(v):
            vx, vy = swap(v, X), swap(v, Y)
            half = rows // 2
            lo = swap(vx[:half], Y)
            hi = swap(vy[half:], X)
            mine = jnp.concatenate([v, vx, vy, lo, hi], axis=0)
            return mine, swap(mine, CORE)

        def pair_gather(v):
            mine = jnp.concatenate([v, swap(v, ZL)], axis=0)
            return mine, swap(mine, CORE)

        def halve(arr, axis, b):
            keep = lax.dynamic_index_in_dim(arr, bit(b), axis, keepdims=False)
            send = lax.dynamic_index_in_dim(arr, 1 - bit(b), axis, keepdims=False)
            return keep + swap(send, b)

        def line_reduce(arr):
            right = [[(i, i + 8) for i in range(n) if i // 8 <= min(s, 2)] for s in range(3)]
            left = [[(i, i - 8) for i in range(n) if 3 - i // 8 <= min(s, 2)] for s in range(3)]
            recv_r = recv_l = None
            for s in range(3):
                send_r = lax.dynamic_index_in_dim(arr, jnp.clip(3 - s + z, 0, 3), 0, keepdims=False)
                send_l = lax.dynamic_index_in_dim(arr, jnp.clip(s + z - 3, 0, 3), 0, keepdims=False)
                if s:
                    send_r, send_l = send_r + recv_r, send_l + recv_l
                recv_r = lax.ppermute(send_r, "data", right[s])
                recv_l = lax.ppermute(send_l, "data", left[s])
            own = lax.dynamic_index_in_dim(arr, z, 0, keepdims=False)
            return own + recv_r + recv_l

        def spread(arr, axis, b):
            keep = lax.dynamic_index_in_dim(arr, bit(b), axis, keepdims=False)
            send = lax.dynamic_index_in_dim(arr, 1 - bit(b), axis, keepdims=False)
            recv = swap(send, b)
            first = jnp.where(bit(b) == 0, keep, recv)
            second = jnp.where(bit(b) == 0, recv, keep)
            return jnp.stack([first, second], axis=axis)

        def share_of(w, axis, owners):
            return jnp.concatenate(
                [lax.dynamic_slice_in_dim(w, o * fr, fr, axis) for o in owners], axis=axis)

        owners1 = [(zh * 16 + y * 4 + x * 2) + bit(ZL) * 8 + bit(CORE)
                   for zh in range(2) for y in range(2) for x in range(2)]
        owners0 = [zz * 8 + idx % 8 for zz in range(4)]

        def act_of(hs, wq):
            pre = [dot(h, wq, ((1,), (0,))).astype(BF16) for h in hs]
            return pre, [gelu_act(p.astype(F32)).astype(BF16) for p in pre]

        def grad_pre_of(pre, grad_act):
            _, pullback = jax.vjp(gelu_act, pre.astype(F32))
            return pullback(grad_act.astype(F32))[0].astype(BF16)

        def summed(lhs, rhs):
            return dot(lhs[0], rhs[0], ((0,), (0,))) + dot(lhs[1], rhs[1], ((0,), (0,)))

        h0s = plane_gather(tokens)
        pre0 = dot(tokens, w_in[0], ((1,), (0,))).astype(BF16)
        act0 = gelu_act(pre0.astype(F32)).astype(BF16)
        h1 = (tokens.astype(F32) + dot(act0, w_out[0], ((1,), (0,)))).astype(BF16)
        h1s = pair_gather(h1)
        pre1 = dot(h1, w_in[1], ((1,), (0,))).astype(BF16)
        act1 = gelu_act(pre1.astype(F32)).astype(BF16)
        h2 = (h1.astype(F32) + dot(act1, w_out[1], ((1,), (0,)))).astype(BF16)
        g1 = ((h2.astype(F32) - targets.astype(F32)) * scale).astype(BF16)
        g1s = pair_gather(g1)
        grad_act1 = dot(g1, w_out[1], ((1,), (1,))).astype(BF16)
        grad_pre1 = grad_pre_of(pre1, grad_act1)
        g0 = (g1.astype(F32) + dot(grad_pre1, w_in[1], ((1,), (1,)))).astype(BF16)
        g0s = plane_gather(g0)

        def share_grads(hs, gs, layer, owners):
            w1 = share_of(w_in[layer], 1, owners)
            w2 = share_of(w_out[layer], 0, owners)
            pre, act = act_of(hs, w1)
            ge = [dot(g, w2, ((1,), (1,))).astype(BF16) for g in gs]
            gp = [grad_pre_of(p, e) for p, e in zip(pre, ge)]
            return summed(hs, gp), summed(act, gs)

        in1, out1 = share_grads(h1s, g1s, 1, owners1)
        out1 = out1.reshape(2, 2, 2, fr, d)
        out1 = halve(halve(halve(out1, 2, X), 1, Y), 0, ZH)
        in1 = in1.reshape(2, 2, 2, 2, 2, dr, 8 * fr)
        in1 = halve(in1, 2, Y)
        in1 = halve(in1, 2, X)
        in1 = halve(in1, 0, ZH)
        in1 = spread(spread(in1, 0, ZL), 1, CORE)
        in1 = in1.reshape(2, 2, dr, 2, 2, 2, fr)
        in1 = in1.transpose(2, 3, 0, 4, 5, 1, 6).reshape(dr, ff)

        in0, out0 = share_grads(h0s, g0s, 0, owners0)
        out0 = line_reduce(out0.reshape(4, fr, d))
        in0 = line_reduce(in0.reshape(4, 8 * dr, 4 * fr))
        in0 = in0.reshape(2, 2, 2, dr, 4 * fr)
        in0 = spread(spread(spread(in0, 0, Y), 1, X), 2, CORE)
        in0 = in0.reshape(8, dr, 4, fr).transpose(1, 2, 0, 3).reshape(dr, ff)
        return jnp.stack([in0, in1]), jnp.stack([out0, out1])

    tok_spec = P("data", None)
    grad_spec = P(None, "data", None)
    return jax.shard_map(local_grads, mesh=mesh, in_specs=(tok_spec, tok_spec, P(), P()), out_specs=(grad_spec, grad_spec), check_vma=False)
```

```python
import jax
import jax.numpy as jnp
from jax import lax
from jax.experimental import pallas as pl
from jax.experimental.pallas import tpu as pltpu
from jax.sharding import PartitionSpec as P


CORE, X, Y, ZL, ZH = 1, 2, 4, 8, 16
F32, BF16 = jnp.float32, jnp.bfloat16


def gelu_act(pre_f32):
    return jax.nn.gelu(pre_f32, approximate=True)


def dot(a, b, dims):
    return lax.dot_general(a, b, (dims, ((), ())), preferred_element_type=F32)


NN, NT, TN = ((1,), (0,)), ((1,), (1,)), ((0,), (0,))
ANY = pl.BlockSpec(memory_space=pl.ANY)
WHOLE = pl.BlockSpec(memory_space=pltpu.VMEM)


def grad_pre_of(pre, grad_act):
    _, pullback = jax.vjp(gelu_act, pre.astype(F32))
    return pullback(grad_act.astype(F32))[0].astype(BF16)


def start_rows(refs, buf, sems, piece):
    k = 0
    for ref in refs:
        for r in range(0, ref.shape[0], piece):
            pltpu.make_async_copy(ref.at[pl.ds(r, piece)], buf.at[pl.ds(k * piece, piece)], sems.at[k]).start()
            k += 1


def wait_rows(buf, sems, piece, tile, i):
    for j in range(tile // piece):
        k = i * (tile // piece) + j
        view = buf.at[pl.ds(k * piece, piece)]
        pltpu.make_async_copy(view, view, sems.at[k]).wait()


def call(kernel, operands, in_specs, out_shape, out_specs, scratch, flops):
    nbytes = sum(o.size * o.dtype.itemsize for o in operands)
    return pl.pallas_call(
        kernel, out_shape=out_shape, in_specs=in_specs, out_specs=out_specs, scratch_shapes=scratch,
        compiler_params=pltpu.CompilerParams(vmem_limit_bytes=62 * 1024 * 1024),
        cost_estimate=pl.CostEstimate(flops=flops, bytes_accessed=nbytes, transcendentals=0),
    )(*operands)


def sizes_of(blocks):
    piece = min(b.shape[0] for b in blocks)
    total = sum(b.shape[0] for b in blocks)
    return piece, total, blocks[0].shape[1]


def share_forward(blocks, w):
    piece, total, d = sizes_of(blocks)
    cols = w.shape[1]
    nb, steps = len(blocks), total // piece

    def kernel(*refs):
        h_refs, (w_ref, pre_ref, act_ref, h_buf, pre_buf, act_buf, sems, out_sems) = refs[:nb], refs[nb:]
        start_rows(h_refs, h_buf, sems, piece)

        def outs(i, slot):
            rows = pl.ds(i * piece, piece)
            return (pltpu.make_async_copy(pre_buf.at[slot], pre_ref.at[rows], out_sems.at[slot, 0]),
                    pltpu.make_async_copy(act_buf.at[slot], act_ref.at[rows], out_sems.at[slot, 1]))

        def step(i, _):
            slot = i % 2
            wait_rows(h_buf, sems, piece, piece, i)

            @pl.when(i >= 2)
            def _():
                for c in outs(i - 2, slot):
                    c.wait()

            pre = dot(h_buf[pl.ds(i * piece, piece), :], w_ref[...], NN).astype(BF16)
            pre_buf[slot] = pre
            act_buf[slot] = gelu_act(pre.astype(F32)).astype(BF16)
            for c in outs(i, slot):
                c.start()
            return 0

        lax.fori_loop(0, steps, step, 0)
        for i in range(max(steps - 2, 0), steps):
            for c in outs(i, i % 2):
                c.wait()

    shape = jax.ShapeDtypeStruct((total, cols), BF16)
    return call(kernel, [*blocks, w], [ANY] * nb + [WHOLE], [shape, shape], [ANY, ANY],
                [pltpu.VMEM((total, d), BF16), pltpu.VMEM((2, piece, cols), BF16), pltpu.VMEM((2, piece, cols), BF16),
                 pltpu.SemaphoreType.DMA((steps,)), pltpu.SemaphoreType.DMA((2, 2))], 2 * total * d * cols)


def share_out(act, blocks):
    piece, total, d = sizes_of(blocks)
    cols = act.shape[1]
    nb, tile = len(blocks), 2 * piece

    def kernel(*refs):
        act_ref, g_refs, (out_ref, act_buf, g_buf, act_sems, sems) = refs[0], refs[1:1 + nb], refs[1 + nb:]
        start_rows([act_ref], act_buf, act_sems, piece)
        start_rows(g_refs, g_buf, sems, piece)
        chunk = cols // 5 if cols % 640 == 0 else cols

        def step(i, _):
            wait_rows(act_buf, act_sems, piece, tile, i)
            wait_rows(g_buf, sems, piece, tile, i)
            rows = pl.ds(i * tile, tile)

            def part(c, _):
                at = pl.ds(pl.multiple_of(c * chunk, chunk), chunk)
                val = dot(act_buf[rows, at], g_buf[rows, :], TN)

                @pl.when(i == 0)
                def _():
                    out_ref[at, :] = val

                @pl.when(i > 0)
                def _():
                    out_ref[at, :] += val
                return 0

            lax.fori_loop(0, cols // chunk, part, 0)
            return 0

        lax.fori_loop(0, total // tile, step, 0)

    return call(kernel, [act, *blocks], [ANY] * (nb + 1), jax.ShapeDtypeStruct((cols, d), F32), WHOLE,
                [pltpu.VMEM((total, cols), BF16), pltpu.VMEM((total, d), BF16),
                 pltpu.SemaphoreType.DMA((total // piece,)), pltpu.SemaphoreType.DMA((total // piece,))],
                2 * total * d * cols)


def share_in(hs, gs, pre, w):
    piece, total, d = sizes_of(hs)
    cols = w.shape[0]
    nb, tile = len(hs), 2 * piece
    steps = total // tile

    def kernel(*refs):
        h_refs, g_refs = refs[:nb], refs[nb:2 * nb]
        pre_ref, w_ref, out_ref, h_buf, g_buf, pre_buf, v_buf, h_sems, g_sems, pre_sems = refs[2 * nb:]
        start_rows(g_refs, g_buf, g_sems, piece)
        start_rows(h_refs, h_buf, h_sems, piece)

        def fetch(i, slot):
            return pltpu.make_async_copy(pre_ref.at[pl.ds(i * tile, tile)], pre_buf.at[slot], pre_sems.at[slot])

        fetch(0, 0).start()
        chunk = d // 5 if d % 640 == 0 else d

        def step(i, _):
            slot = i % 2
            wait_rows(g_buf, g_sems, piece, tile, i)
            wait_rows(h_buf, h_sems, piece, tile, i)
            fetch(i, slot).wait()

            @pl.when(i + 1 < steps)
            def _():
                fetch(i + 1, 1 - slot).start()

            def head(j, _):
                sub = pl.ds(j * piece, piece)
                e = dot(g_buf[pl.ds(i * tile + j * piece, piece), :], w_ref[...], NT).astype(BF16)
                v_buf[sub, :] = grad_pre_of(pre_buf[slot, sub, :], e)
                return 0

            lax.fori_loop(0, 2, head, 0)
            rows = pl.ds(i * tile, tile)

            def part(c, _):
                at = pl.ds(pl.multiple_of(c * chunk, chunk), chunk)
                val = dot(h_buf[rows, at], v_buf[...], TN)

                @pl.when(i == 0)
                def _():
                    out_ref[at, :] = val

                @pl.when(i > 0)
                def _():
                    out_ref[at, :] += val
                return 0

            lax.fori_loop(0, d // chunk, part, 0)
            return 0

        lax.fori_loop(0, steps, step, 0)

    n_sem = total // piece
    return call(kernel, [*hs, *gs, pre, w], [ANY] * (2 * nb + 1) + [WHOLE], jax.ShapeDtypeStruct((d, cols), F32), WHOLE,
                [pltpu.VMEM((total, d), BF16), pltpu.VMEM((total, d), BF16), pltpu.VMEM((2, tile, cols), BF16),
                 pltpu.VMEM((tile, cols), BF16), pltpu.SemaphoreType.DMA((n_sem,)), pltpu.SemaphoreType.DMA((n_sem,)),
                 pltpu.SemaphoreType.DMA((2,))], 4 * total * d * cols)


def solution(mesh):
    n = mesh.shape["data"]

    def swap(v, bit):
        return lax.ppermute(v, "data", [(i, i ^ bit) for i in range(n)])

    def local_grads(tokens, targets, w_in, w_out):
        rows, d = tokens.shape
        ff = w_in.shape[2]
        dr, fr = d // n, ff // n
        scale = (rows * n) ** -0.5
        idx = lax.axis_index("data")

        def bit(b):
            return (idx // b) % 2

        z = idx // 8

        def plane_gather(v):
            vx, vy = swap(v, X), swap(v, Y)
            half = rows // 2
            lo = swap(vx[:half], Y)
            hi = swap(vy[half:], X)
            mine = [v, vx, vy, lo, hi]
            return mine + [swap(m, CORE) for m in mine]

        def pair_gather(v):
            mine = [v, swap(v, ZL)]
            return mine + [swap(m, CORE) for m in mine]

        def halve(arr, axis, b):
            keep = lax.dynamic_index_in_dim(arr, bit(b), axis, keepdims=False)
            send = lax.dynamic_index_in_dim(arr, 1 - bit(b), axis, keepdims=False)
            return keep + swap(send, b)

        def line_reduce(arr):
            right = [[(i, i + 8) for i in range(n) if i // 8 <= min(s, 2)] for s in range(3)]
            left = [[(i, i - 8) for i in range(n) if 3 - i // 8 <= min(s, 2)] for s in range(3)]
            recv_r = recv_l = None
            for s in range(3):
                send_r = lax.dynamic_index_in_dim(arr, jnp.clip(3 - s + z, 0, 3), 0, keepdims=False)
                send_l = lax.dynamic_index_in_dim(arr, jnp.clip(s + z - 3, 0, 3), 0, keepdims=False)
                if s:
                    send_r, send_l = send_r + recv_r, send_l + recv_l
                recv_r = lax.ppermute(send_r, "data", right[s])
                recv_l = lax.ppermute(send_l, "data", left[s])
            own = lax.dynamic_index_in_dim(arr, z, 0, keepdims=False)
            return own + recv_r + recv_l

        def spread(arr, axis, b):
            keep = lax.dynamic_index_in_dim(arr, bit(b), axis, keepdims=False)
            send = lax.dynamic_index_in_dim(arr, 1 - bit(b), axis, keepdims=False)
            recv = swap(send, b)
            first = jnp.where(bit(b) == 0, keep, recv)
            second = jnp.where(bit(b) == 0, recv, keep)
            return jnp.stack([first, second], axis=axis)

        def share_of(w, layer, axis, owners):
            start = lambda o: (layer, o * fr, 0) if axis == 0 else (layer, 0, o * fr)
            size = (1, fr, d) if axis == 0 else (1, d, fr)
            return jnp.concatenate([lax.dynamic_slice(w, start(o), size)[0] for o in owners], axis=axis)

        owners1 = [(zh * 16 + y * 4 + x * 2) + bit(ZL) * 8 + bit(CORE)
                   for zh in range(2) for y in range(2) for x in range(2)]
        owners0 = [zz * 8 + idx % 8 for zz in range(4)]

        h0s = plane_gather(tokens)
        pre0 = dot(tokens, w_in[0], ((1,), (0,))).astype(BF16)
        act0 = gelu_act(pre0.astype(F32)).astype(BF16)
        h1 = (tokens.astype(F32) + dot(act0, w_out[0], ((1,), (0,)))).astype(BF16)
        h1s = pair_gather(h1)
        pre1 = dot(h1, w_in[1], ((1,), (0,))).astype(BF16)
        act1 = gelu_act(pre1.astype(F32)).astype(BF16)
        h2 = (h1.astype(F32) + dot(act1, w_out[1], ((1,), (0,)))).astype(BF16)
        g1 = ((h2.astype(F32) - targets.astype(F32)) * scale).astype(BF16)
        g1s = pair_gather(g1)
        grad_act1 = dot(g1, w_out[1], ((1,), (1,))).astype(BF16)
        grad_pre1 = grad_pre_of(pre1, grad_act1)
        g0 = (g1.astype(F32) + dot(grad_pre1, w_in[1], ((1,), (1,)))).astype(BF16)
        g0s = plane_gather(g0)

        pre1s, act1s = share_forward(h1s, share_of(w_in, 1, 1, owners1))
        pre0s, act0s = share_forward(h0s, share_of(w_in, 0, 1, owners0))
        out1 = share_out(act1s, g1s)
        in1 = share_in(h1s, g1s, pre1s, share_of(w_out, 1, 0, owners1))
        out0 = share_out(act0s, g0s)
        in0 = share_in(h0s, g0s, pre0s, share_of(w_out, 0, 0, owners0))

        out1 = out1.reshape(2, 2, 2, fr, d)
        out1 = halve(halve(halve(out1, 2, X), 1, Y), 0, ZH)
        in1 = in1.reshape(2, 2, 2, 2, 2, dr, 8 * fr)
        in1 = halve(in1, 2, Y)
        in1 = halve(in1, 2, X)
        in1 = halve(in1, 0, ZH)
        in1 = spread(spread(in1, 0, ZL), 1, CORE)
        in1 = in1.reshape(2, 2, dr, 2, 2, 2, fr)
        in1 = in1.transpose(2, 3, 0, 4, 5, 1, 6).reshape(dr, ff)

        out0 = line_reduce(out0.reshape(4, fr, d))
        in0 = line_reduce(in0.reshape(4, 8 * dr, 4 * fr))
        in0 = in0.reshape(2, 2, 2, dr, 4 * fr)
        in0 = spread(spread(spread(in0, 0, Y), 1, X), 2, CORE)
        in0 = in0.reshape(8, dr, 4, fr).transpose(1, 2, 0, 3).reshape(dr, ff)
        return jnp.stack([in0, in1]), jnp.stack([out0, out1])

    tok_spec = P("data", None)
    grad_spec = P(None, "data", None)
    return jax.shard_map(local_grads, mesh=mesh, in_specs=(tok_spec, tok_spec, P(), P()), out_specs=(grad_spec, grad_spec), check_vma=False)
```

```python
import jax
import jax.numpy as jnp
from jax import lax
from jax.experimental import pallas as pl
from jax.experimental.pallas import tpu as pltpu
from jax.sharding import PartitionSpec as P


CORE, X, Y, ZL, ZH = 1, 2, 4, 8, 16
F32, BF16 = jnp.float32, jnp.bfloat16


def gelu_act(pre_f32):
    return jax.nn.gelu(pre_f32, approximate=True)


def dot(a, b, dims):
    return lax.dot_general(a, b, (dims, ((), ())), preferred_element_type=F32)


NN, NT, TN = ((1,), (0,)), ((1,), (1,)), ((0,), (0,))
ANY = pl.BlockSpec(memory_space=pl.ANY)
WHOLE = pl.BlockSpec(memory_space=pltpu.VMEM)


def grad_pre_of(pre, grad_act):
    _, pullback = jax.vjp(gelu_act, pre.astype(F32))
    return pullback(grad_act.astype(F32))[0].astype(BF16)


def start_rows(refs, buf, sems, piece):
    k = 0
    for ref in refs:
        for r in range(0, ref.shape[0], piece):
            pltpu.make_async_copy(ref.at[pl.ds(r, piece)], buf.at[pl.ds(k * piece, piece)], sems.at[k]).start()
            k += 1


def wait_rows(buf, sems, piece, tile, i):
    for j in range(tile // piece):
        k = i * (tile // piece) + j
        view = buf.at[pl.ds(k * piece, piece)]
        pltpu.make_async_copy(view, view, sems.at[k]).wait()


def call(kernel, operands, in_specs, out_shape, out_specs, scratch, flops):
    nbytes = sum(o.size * o.dtype.itemsize for o in operands)
    return pl.pallas_call(
        kernel, out_shape=out_shape, in_specs=in_specs, out_specs=out_specs, scratch_shapes=scratch,
        compiler_params=pltpu.CompilerParams(vmem_limit_bytes=62 * 1024 * 1024),
        cost_estimate=pl.CostEstimate(flops=flops, bytes_accessed=nbytes, transcendentals=0),
    )(*operands)


def sizes_of(blocks):
    piece = min(b.shape[0] for b in blocks)
    total = sum(b.shape[0] for b in blocks)
    return piece, total, blocks[0].shape[1]


def share_forward(blocks, w):
    piece, total, d = sizes_of(blocks)
    cols = w.shape[1]
    nb, steps = len(blocks), total // piece

    def kernel(*refs):
        h_refs, (w_ref, pre_ref, act_ref, h_buf, pre_buf, act_buf, sems, out_sems) = refs[:nb], refs[nb:]
        start_rows(h_refs, h_buf, sems, piece)

        def outs(i, slot):
            rows = pl.ds(i * piece, piece)
            return (pltpu.make_async_copy(pre_buf.at[slot], pre_ref.at[rows], out_sems.at[slot, 0]),
                    pltpu.make_async_copy(act_buf.at[slot], act_ref.at[rows], out_sems.at[slot, 1]))

        def step(i, _):
            slot = i % 2
            wait_rows(h_buf, sems, piece, piece, i)

            @pl.when(i >= 2)
            def _():
                for c in outs(i - 2, slot):
                    c.wait()

            pre = dot(h_buf[pl.ds(i * piece, piece), :], w_ref[...], NN).astype(BF16)
            pre_buf[slot] = pre
            act_buf[slot] = gelu_act(pre.astype(F32)).astype(BF16)
            for c in outs(i, slot):
                c.start()
            return 0

        lax.fori_loop(0, steps, step, 0)
        for i in range(max(steps - 2, 0), steps):
            for c in outs(i, i % 2):
                c.wait()

    shape = jax.ShapeDtypeStruct((total, cols), BF16)
    return call(kernel, [*blocks, w], [ANY] * nb + [WHOLE], [shape, shape], [ANY, ANY],
                [pltpu.VMEM((total, d), BF16), pltpu.VMEM((2, piece, cols), BF16), pltpu.VMEM((2, piece, cols), BF16),
                 pltpu.SemaphoreType.DMA((steps,)), pltpu.SemaphoreType.DMA((2, 2))], 2 * total * d * cols)


def share_out(act, blocks):
    piece, total, d = sizes_of(blocks)
    cols = act.shape[1]
    nb, tile = len(blocks), 2 * piece

    def kernel(*refs):
        act_ref, g_refs, (out_ref, act_buf, g_buf, act_sems, sems) = refs[0], refs[1:1 + nb], refs[1 + nb:]
        start_rows([act_ref], act_buf, act_sems, piece)
        start_rows(g_refs, g_buf, sems, piece)
        chunk = cols // 5 if cols % 640 == 0 else cols

        def step(i, _):
            wait_rows(act_buf, act_sems, piece, tile, i)
            wait_rows(g_buf, sems, piece, tile, i)
            rows = pl.ds(i * tile, tile)

            def part(c, _):
                at = pl.ds(pl.multiple_of(c * chunk, chunk), chunk)
                val = dot(act_buf[rows, at], g_buf[rows, :], TN)

                @pl.when(i == 0)
                def _():
                    out_ref[at, :] = val

                @pl.when(i > 0)
                def _():
                    out_ref[at, :] += val

                return 0

            lax.fori_loop(0, cols // chunk, part, 0)
            return 0

        lax.fori_loop(0, total // tile, step, 0)

    return call(kernel, [act, *blocks], [ANY] * (nb + 1), jax.ShapeDtypeStruct((cols, d), F32), WHOLE,
                [pltpu.VMEM((total, cols), BF16), pltpu.VMEM((total, d), BF16),
                 pltpu.SemaphoreType.DMA((total // piece,)), pltpu.SemaphoreType.DMA((total // piece,))],
                2 * total * d * cols)


def share_in(hs, gs, pre, w):
    piece, total, d = sizes_of(hs)
    cols = w.shape[0]
    nb, tile = len(hs), 2 * piece
    steps = total // tile

    def kernel(*refs):
        h_refs, g_refs = refs[:nb], refs[nb:2 * nb]
        pre_ref, w_ref, out_ref, h_buf, g_buf, pre_buf, v_buf, h_sems, g_sems, pre_sems = refs[2 * nb:]
        start_rows(g_refs, g_buf, g_sems, piece)
        start_rows(h_refs, h_buf, h_sems, piece)

        def fetch(i, slot):
            return pltpu.make_async_copy(pre_ref.at[pl.ds(i * tile, tile)], pre_buf.at[slot], pre_sems.at[slot])

        fetch(0, 0).start()
        chunk = d // 5 if d % 640 == 0 else d

        def step(i, _):
            slot = i % 2
            wait_rows(g_buf, g_sems, piece, tile, i)
            wait_rows(h_buf, h_sems, piece, tile, i)
            fetch(i, slot).wait()

            @pl.when(i + 1 < steps)
            def _():
                fetch(i + 1, 1 - slot).start()

            def head(j, _):
                sub = pl.ds(j * piece, piece)
                e = dot(g_buf[pl.ds(i * tile + j * piece, piece), :], w_ref[...], NT).astype(BF16)
                v_buf[sub, :] = grad_pre_of(pre_buf[slot, sub, :], e)
                return 0

            lax.fori_loop(0, 2, head, 0)
            rows = pl.ds(i * tile, tile)

            def part(c, _):
                at = pl.ds(pl.multiple_of(c * chunk, chunk), chunk)
                val = dot(h_buf[rows, at], v_buf[...], TN)

                @pl.when(i == 0)
                def _():
                    out_ref[at, :] = val

                @pl.when(i > 0)
                def _():
                    out_ref[at, :] += val

                return 0

            lax.fori_loop(0, d // chunk, part, 0)
            return 0

        lax.fori_loop(0, steps, step, 0)

    n_sem = total // piece
    return call(kernel, [*hs, *gs, pre, w], [ANY] * (2 * nb + 1) + [WHOLE], jax.ShapeDtypeStruct((d, cols), F32), WHOLE,
                [pltpu.VMEM((total, d), BF16), pltpu.VMEM((total, d), BF16), pltpu.VMEM((2, tile, cols), BF16),
                 pltpu.VMEM((tile, cols), BF16), pltpu.SemaphoreType.DMA((n_sem,)), pltpu.SemaphoreType.DMA((n_sem,)),
                 pltpu.SemaphoreType.DMA((2,))], 4 * total * d * cols)


def solution(mesh):
    n = mesh.shape["data"]

    def permute(v, pairs):
        return lax.ppermute(v, "data", pairs)

    def swap(v, bit):
        return permute(v, [(i, i ^ bit) for i in range(n)])

    def local_grads(tokens, targets, w_in, w_out):
        rows, d = tokens.shape
        ff = w_in.shape[2]
        dr, fr = d // n, ff // n
        scale = (rows * n) ** -0.5
        idx = lax.axis_index("data")

        def bit(b):
            return (idx // b) % 2

        z = idx // 8

        def plane_gather(v):
            vx, vy = swap(v, X), swap(v, Y)
            half = rows // 2
            lo = swap(vx[:half], Y)
            hi = swap(vy[half:], X)
            mine = [v, vx, vy, lo, hi]
            return mine + [swap(m, CORE) for m in mine]

        def pair_gather(v):
            mine = [v, swap(v, ZL)]
            return mine + [swap(m, CORE) for m in mine]

        def halve(arr, axis, b):
            keep = lax.dynamic_index_in_dim(arr, bit(b), axis, keepdims=False)
            send = lax.dynamic_index_in_dim(arr, 1 - bit(b), axis, keepdims=False)
            return keep + swap(send, b)

        def line_reduce(arr):
            right = [[(i, i + 8) for i in range(n) if i // 8 <= min(s, 2)] for s in range(3)]
            left = [[(i, i - 8) for i in range(n) if 3 - i // 8 <= min(s, 2)] for s in range(3)]
            recv_r = recv_l = None
            for s in range(3):
                send_r = lax.dynamic_index_in_dim(arr, jnp.clip(3 - s + z, 0, 3), 0, keepdims=False)
                send_l = lax.dynamic_index_in_dim(arr, jnp.clip(s + z - 3, 0, 3), 0, keepdims=False)
                if s:
                    send_r, send_l = send_r + recv_r, send_l + recv_l
                recv_r = permute(send_r, right[s])
                recv_l = permute(send_l, left[s])
            own = lax.dynamic_index_in_dim(arr, z, 0, keepdims=False)
            return own + recv_r + recv_l

        def spread(arr, axis, b):
            keep = lax.dynamic_index_in_dim(arr, bit(b), axis, keepdims=False)
            send = lax.dynamic_index_in_dim(arr, 1 - bit(b), axis, keepdims=False)
            recv = swap(send, b)
            first = jnp.where(bit(b) == 0, keep, recv)
            second = jnp.where(bit(b) == 0, recv, keep)
            return jnp.stack([first, second], axis=axis)

        def share_of(w, layer, axis, owners):
            start = lambda o: (layer, o * fr, 0) if axis == 0 else (layer, 0, o * fr)
            size = (1, fr, d) if axis == 0 else (1, d, fr)
            return jnp.concatenate([lax.dynamic_slice(w, start(o), size)[0] for o in owners], axis=axis)

        owners1 = [(zh * 16 + y * 4 + x * 2) + bit(ZL) * 8 + bit(CORE)
                   for zh in range(2) for y in range(2) for x in range(2)]
        owners0 = [zz * 8 + idx % 8 for zz in range(4)]

        h0s = plane_gather(tokens)
        pre0 = dot(tokens, w_in[0], NN).astype(BF16)
        act0 = gelu_act(pre0.astype(F32)).astype(BF16)
        h1 = (tokens.astype(F32) + dot(act0, w_out[0], NN)).astype(BF16)
        h1s = pair_gather(h1)
        pre1 = dot(h1, w_in[1], NN).astype(BF16)
        act1 = gelu_act(pre1.astype(F32)).astype(BF16)
        h2 = (h1.astype(F32) + dot(act1, w_out[1], NN)).astype(BF16)
        g1 = ((h2.astype(F32) - targets.astype(F32)) * scale).astype(BF16)
        g1s = pair_gather(g1)
        grad_act1 = dot(g1, w_out[1], NT).astype(BF16)
        grad_pre1 = grad_pre_of(pre1, grad_act1)
        g0 = (g1.astype(F32) + dot(grad_pre1, w_in[1], NT)).astype(BF16)
        g0s = plane_gather(g0)

        w_in1, w_in0 = share_of(w_in, 1, 1, owners1), share_of(w_in, 0, 1, owners0)
        w_out1, w_out0 = share_of(w_out, 1, 0, owners1), share_of(w_out, 0, 0, owners0)
        pre1s, act1s = share_forward(h1s, w_in1)
        pre0s, act0s = share_forward(h0s, w_in0)
        out1 = share_out(act1s, g1s)
        in1 = share_in(h1s, g1s, pre1s, w_out1)
        in0 = share_in(h0s, g0s, pre0s, w_out0)
        out0 = share_out(act0s, g0s)

        out1 = out1.reshape(2, 2, 2, fr, d)
        out1 = halve(out1, 2, X)
        out1 = halve(out1, 1, Y)
        out1 = halve(out1, 0, ZH)
        in1 = in1.reshape(2, 2, 2, 2, 2, dr, 8 * fr)
        in1 = halve(in1, 2, Y)
        in1 = halve(in1, 2, X)
        in1 = halve(in1, 0, ZH)
        in1 = spread(spread(in1, 0, ZL), 1, CORE)
        in1 = in1.reshape(2, 2, dr, 2, 2, 2, fr)
        in1 = in1.transpose(2, 3, 0, 4, 5, 1, 6).reshape(dr, ff)

        out0 = line_reduce(out0.reshape(4, fr, d))
        in0 = line_reduce(in0.reshape(4, 8 * dr, 4 * fr))
        in0 = in0.reshape(2, 2, 2, dr, 4 * fr)
        in0 = spread(spread(spread(in0, 0, Y), 1, X), 2, CORE)
        in0 = in0.reshape(8, dr, 4, fr).transpose(1, 2, 0, 3).reshape(dr, ff)
        return jnp.stack([in0, in1]), jnp.stack([out0, out1])

    tok_spec = P("data", None)
    grad_spec = P(None, "data", None)
    return jax.shard_map(local_grads, mesh=mesh, in_specs=(tok_spec, tok_spec, P(), P()), out_specs=(grad_spec, grad_spec), check_vma=False)
```

```python
import jax
import jax.numpy as jnp
from jax import lax
from jax.experimental import pallas as pl
from jax.experimental.pallas import tpu as pltpu
from jax.sharding import PartitionSpec as P


CORE, X, Y, ZL, ZH = 1, 2, 4, 8, 16
F32, BF16 = jnp.float32, jnp.bfloat16


OUT_ROUTES = {"a": (4, (2, 4, 16)), "b": (3, (4, 2, 16)), "c": (3, (16, 2, 4))}
IN_ROUTES = {"a": (5, (4, 2, 16)), "b": (5, (2, 4, 16))}


def gelu_act(pre_f32):
    return jax.nn.gelu(pre_f32, approximate=True)


def dot(a, b, dims):
    return lax.dot_general(a, b, (dims, ((), ())), preferred_element_type=F32)


NN, NT, TN = ((1,), (0,)), ((1,), (1,)), ((0,), (0,))
ANY = pl.BlockSpec(memory_space=pl.ANY)
WHOLE = pl.BlockSpec(memory_space=pltpu.VMEM)


def grad_pre_of(pre, grad_act):
    _, pullback = jax.vjp(gelu_act, pre.astype(F32))
    return pullback(grad_act.astype(F32))[0].astype(BF16)


def start_rows(*streams, piece):
    todo = [[(ref, r, buf, sems) for ref in refs for r in range(0, ref.shape[0], piece)] for refs, buf, sems in streams]
    for k in range(len(todo[0])):
        for stream in todo:
            ref, r, buf, sems = stream[k]
            pltpu.make_async_copy(ref.at[pl.ds(r, piece)], buf.at[pl.ds(k * piece, piece)], sems.at[k]).start()


def wait_rows(buf, sems, piece, tile, i):
    for j in range(tile // piece):
        k = i * (tile // piece) + j
        view = buf.at[pl.ds(k * piece, piece)]
        pltpu.make_async_copy(view, view, sems.at[k]).wait()


def call(kernel, operands, in_specs, out_shape, out_specs, scratch, flops):
    nbytes = sum(o.size * o.dtype.itemsize for o in operands)
    return pl.pallas_call(
        kernel, out_shape=out_shape, in_specs=in_specs, out_specs=out_specs, scratch_shapes=scratch,
        compiler_params=pltpu.CompilerParams(vmem_limit_bytes=63 * 1024 * 1024),
        cost_estimate=pl.CostEstimate(flops=flops, bytes_accessed=nbytes, transcendentals=0),
    )(*operands)


def accumulate(i, steps, n_parts, chunk, part_of, acc, out_ref, out_sems):
    def part(c, _):
        at = pl.ds(pl.multiple_of(c * chunk, chunk), chunk)
        val = part_of(at)

        @pl.when(i == 0)
        def _():
            acc[at, :] = val

        @pl.when(i > 0)
        def _():
            acc[at, :] += val

        @pl.when(i == steps - 1)
        def _():
            pltpu.make_async_copy(acc.at[at], out_ref.at[at], out_sems.at[c]).start()

        return 0

    lax.fori_loop(0, n_parts, part, 0)


def finish(n_parts, chunk, acc, out_ref, out_sems):
    for c in range(n_parts):
        at = pl.ds(c * chunk, chunk)
        pltpu.make_async_copy(acc.at[at], out_ref.at[at], out_sems.at[c]).wait()


def sizes_of(blocks):
    piece = min(b.shape[0] for b in blocks)
    total = sum(b.shape[0] for b in blocks)
    return piece, total, blocks[0].shape[1]


def share_forward(blocks, w_in, layer, owners_of, fr):
    piece, total, d = sizes_of(blocks)
    piece = min(piece, 512)
    ff = w_in.shape[2]
    count = len(owners_of(jnp.int32(0)))
    cols, wide = count * fr, min(256, ff)
    nb, steps = len(blocks), total // piece

    def kernel(*refs):
        h_refs, (w_ref, pre_ref, act_ref, h_buf, win, w_buf, pre_buf, act_buf, sems, w_sems, out_sems) = refs[:nb], refs[nb:]
        owners = owners_of(lax.axis_index("data"))
        starts = [jnp.minimum((o * fr) // 128 * 128, ff - wide) for o in owners]
        for k, at in enumerate(starts):
            pltpu.make_async_copy(w_ref.at[layer, :, pl.ds(pl.multiple_of(at, 128), wide)], win.at[k], w_sems.at[k]).start()
        start_rows((h_refs, h_buf, sems), piece=piece)
        row = lax.broadcasted_iota(jnp.int32, (wide, fr), 0)
        col = lax.broadcasted_iota(jnp.int32, (wide, fr), 1)
        for k, (o, at) in enumerate(zip(owners, starts)):
            pltpu.make_async_copy(win.at[k], win.at[k], w_sems.at[k]).wait()
            pick = jnp.where(row == col + (o * fr - at), 1.0, 0.0).astype(BF16)
            w_buf[:, k * fr:(k + 1) * fr] = dot(win[k], pick, NN).astype(BF16)

        def outs(i, slot):
            rows = pl.ds(i * piece, piece)
            return (pltpu.make_async_copy(pre_buf.at[slot], pre_ref.at[rows], out_sems.at[slot, 0]),
                    pltpu.make_async_copy(act_buf.at[slot], act_ref.at[rows], out_sems.at[slot, 1]))

        def step(i, _):
            slot = i % 2
            wait_rows(h_buf, sems, piece, piece, i)

            @pl.when(i >= 2)
            def _():
                for c in outs(i - 2, slot):
                    c.wait()

            pre = dot(h_buf[pl.ds(i * piece, piece), :], w_buf[...], NN).astype(BF16)
            pre_buf[slot] = pre
            act_buf[slot] = gelu_act(pre.astype(F32)).astype(BF16)
            for c in outs(i, slot):
                c.start()
            return 0

        lax.fori_loop(0, steps, step, 0)
        for i in range(max(steps - 2, 0), steps):
            for c in outs(i, i % 2):
                c.wait()

    shape = jax.ShapeDtypeStruct((total, cols), BF16)
    return call(kernel, [*blocks, w_in], [ANY] * (nb + 1), [shape, shape], [ANY, ANY],
                [pltpu.VMEM((total, d), BF16), pltpu.VMEM((count, d, wide), BF16), pltpu.VMEM((d, cols), BF16),
                 pltpu.VMEM((2, piece, cols), BF16), pltpu.VMEM((2, piece, cols), BF16),
                 pltpu.SemaphoreType.DMA((steps,)), pltpu.SemaphoreType.DMA((count,)), pltpu.SemaphoreType.DMA((2, 2))],
                2 * total * d * cols)


def share_out(act, blocks):
    piece, total, d = sizes_of(blocks)
    piece = min(piece, 512)
    cols = act.shape[1]
    nb, tile = len(blocks), 2 * piece
    steps = total // tile
    n_parts = 5 if cols % 640 == 0 else 1
    chunk = cols // n_parts

    def kernel(*refs):
        act_ref, g_refs, (out_ref, act_buf, g_buf, acc, act_sems, sems, out_sems) = refs[0], refs[1:1 + nb], refs[1 + nb:]
        start_rows(([act_ref], act_buf, act_sems), (g_refs, g_buf, sems), piece=piece)

        def step(i, _):
            wait_rows(act_buf, act_sems, piece, tile, i)
            wait_rows(g_buf, sems, piece, tile, i)
            rows = pl.ds(i * tile, tile)
            accumulate(i, steps, n_parts, chunk, lambda at: dot(act_buf[rows, at], g_buf[rows, :], TN), acc, out_ref, out_sems)
            return 0

        lax.fori_loop(0, steps, step, 0)
        finish(n_parts, chunk, acc, out_ref, out_sems)

    return call(kernel, [act, *blocks], [ANY] * (nb + 1), jax.ShapeDtypeStruct((cols, d), F32), ANY,
                [pltpu.VMEM((total, cols), BF16), pltpu.VMEM((total, d), BF16), pltpu.VMEM((cols, d), F32),
                 pltpu.SemaphoreType.DMA((total // piece,)), pltpu.SemaphoreType.DMA((total // piece,)),
                 pltpu.SemaphoreType.DMA((n_parts,))],
                2 * total * d * cols)


def share_in(hs, gs, pre, w_out, layer, owners_of, fr):
    piece, total, d = sizes_of(hs)
    piece = min(piece, 512)
    cols = pre.shape[1]
    count = cols // fr
    nb, tile = len(hs), 2 * piece
    steps = total // tile
    n_parts = 5 if d % 640 == 0 else 1
    chunk = d // n_parts

    def kernel(*refs):
        h_refs, g_refs = refs[:nb], refs[nb:2 * nb]
        (pre_ref, w_ref, out_ref, h_buf, g_buf, pre_buf, v_buf, w_buf, acc,
         h_sems, g_sems, pre_sems, w_sems, out_sems) = refs[2 * nb:]
        copies = [pltpu.make_async_copy(w_ref.at[layer, pl.ds(pl.multiple_of(o * fr, fr), fr)],
                                        w_buf.at[pl.ds(k * fr, fr)], w_sems.at[k])
                  for k, o in enumerate(owners_of(lax.axis_index("data")))]
        for c in copies:
            c.start()

        def fetch(i, slot):
            return pltpu.make_async_copy(pre_ref.at[pl.ds(i * tile, tile)], pre_buf.at[slot], pre_sems.at[slot])

        fetch(0, 0).start()
        start_rows((g_refs, g_buf, g_sems), (h_refs, h_buf, h_sems), piece=piece)
        for c in copies:
            c.wait()

        def step(i, _):
            slot = i % 2
            wait_rows(g_buf, g_sems, piece, tile, i)
            fetch(i, slot).wait()

            @pl.when(i + 1 < steps)
            def _():
                fetch(i + 1, 1 - slot).start()

            def head(j, _):
                sub = pl.ds(j * piece, piece)
                e = dot(g_buf[pl.ds(i * tile + j * piece, piece), :], w_buf[...], NT).astype(BF16)
                v_buf[sub, :] = grad_pre_of(pre_buf[slot, sub, :], e)
                return 0

            lax.fori_loop(0, 2, head, 0)
            wait_rows(h_buf, h_sems, piece, tile, i)
            rows = pl.ds(i * tile, tile)
            accumulate(i, steps, n_parts, chunk, lambda at: dot(h_buf[rows, at], v_buf[...], TN), acc, out_ref, out_sems)
            return 0

        lax.fori_loop(0, steps, step, 0)
        finish(n_parts, chunk, acc, out_ref, out_sems)

    n_sem = total // piece
    return call(kernel, [*hs, *gs, pre, w_out], [ANY] * (2 * nb + 2), jax.ShapeDtypeStruct((d, cols), F32), ANY,
                [pltpu.VMEM((total, d), BF16), pltpu.VMEM((total, d), BF16), pltpu.VMEM((2, tile, cols), BF16),
                 pltpu.VMEM((tile, cols), BF16), pltpu.VMEM((cols, d), BF16), pltpu.VMEM((d, cols), F32),
                 pltpu.SemaphoreType.DMA((n_sem,)), pltpu.SemaphoreType.DMA((n_sem,)),
                 pltpu.SemaphoreType.DMA((2,)), pltpu.SemaphoreType.DMA((count,)), pltpu.SemaphoreType.DMA((n_parts,))],
                4 * total * d * cols)


def solution(mesh):
    n = mesh.shape["data"]

    def permute(v, pairs):
        return lax.ppermute(v, "data", pairs)

    def swap(v, bit):
        return permute(v, [(i, i ^ bit) for i in range(n)])

    def local_grads(tokens, targets, w_in, w_out):
        rows, d = tokens.shape
        ff = w_in.shape[2]
        dr, fr = d // n, ff // n
        scale = (rows * n) ** -0.5
        idx = lax.axis_index("data")

        def bit(b):
            return (idx // b) % 2

        z = idx // 8

        def plane_gather(v):
            vx, vy = swap(v, X), swap(v, Y)
            half = rows // 2
            lo = swap(vx[:half], Y)
            hi = swap(vy[half:], X)
            mine = [v, vx, vy, lo, hi]
            return mine + [swap(m, CORE) for m in mine]

        def pair_gather(v):
            mine = [v, swap(v, ZL)]
            return mine + [swap(m, CORE) for m in mine]

        def halve(arr, axis, b):
            keep = lax.dynamic_index_in_dim(arr, bit(b), axis, keepdims=False)
            send = lax.dynamic_index_in_dim(arr, 1 - bit(b), axis, keepdims=False)
            return keep + swap(send, b)

        def line_reduce(arr):
            right = [[(i, i + 8) for i in range(n) if i // 8 <= min(s, 2)] for s in range(3)]
            left = [[(i, i - 8) for i in range(n) if 3 - i // 8 <= min(s, 2)] for s in range(3)]
            recv_r = recv_l = None
            for s in range(3):
                send_r = lax.dynamic_index_in_dim(arr, jnp.clip(3 - s + z, 0, 3), 0, keepdims=False)
                send_l = lax.dynamic_index_in_dim(arr, jnp.clip(s + z - 3, 0, 3), 0, keepdims=False)
                if s:
                    send_r, send_l = send_r + recv_r, send_l + recv_l
                recv_r = permute(send_r, right[s])
                recv_l = permute(send_l, left[s])
            own = lax.dynamic_index_in_dim(arr, z, 0, keepdims=False)
            return own + recv_r + recv_l

        def spread(arr, axis, b):
            keep = lax.dynamic_index_in_dim(arr, bit(b), axis, keepdims=False)
            send = lax.dynamic_index_in_dim(arr, 1 - bit(b), axis, keepdims=False)
            recv = swap(send, b)
            first = jnp.where(bit(b) == 0, keep, recv)
            second = jnp.where(bit(b) == 0, recv, keep)
            return jnp.stack([first, second], axis=axis)

        def scatter(arr, names, routes):
            width, at, parts = arr.shape[-1], 0, []
            for (tenths, order) in routes.values():
                size = width * tenths // 10
                part, left = lax.slice_in_dim(arr, at, at + size, axis=arr.ndim - 1), list(names)
                for b in order:
                    part = halve(part, left.index(b), b)
                    left.remove(b)
                parts.append(part)
                at += size
            return jnp.concatenate(parts, axis=-1)

        def owners1(i):
            return [zh * 16 + y * 4 + x * 2 + (i // ZL) % 2 * 8 + i % 2 for zh in range(2) for y in range(2) for x in range(2)]

        def owners0(i):
            return [zz * 8 + i % 8 for zz in range(4)]

        h0s = plane_gather(tokens)
        pre0 = dot(tokens, w_in[0], NN).astype(BF16)
        act0 = gelu_act(pre0.astype(F32)).astype(BF16)
        h1 = (tokens.astype(F32) + dot(act0, w_out[0], NN)).astype(BF16)
        h1s = pair_gather(h1)
        pre1 = dot(h1, w_in[1], NN).astype(BF16)
        act1 = gelu_act(pre1.astype(F32)).astype(BF16)
        h2 = (h1.astype(F32) + dot(act1, w_out[1], NN)).astype(BF16)
        g1 = ((h2.astype(F32) - targets.astype(F32)) * scale).astype(BF16)
        g1s = pair_gather(g1)
        grad_act1 = dot(g1, w_out[1], NT).astype(BF16)
        grad_pre1 = grad_pre_of(pre1, grad_act1)
        g0 = (g1.astype(F32) + dot(grad_pre1, w_in[1], NT)).astype(BF16)
        g0s = plane_gather(g0)

        pre1s, act1s = share_forward(h1s, w_in, 1, owners1, fr)
        pre0s, act0s = share_forward(h0s, w_in, 0, owners0, fr)
        out1 = share_out(act1s, g1s)
        in1 = share_in(h1s, g1s, pre1s, w_out, 1, owners1, fr)
        out0 = share_out(act0s, g0s)
        in0 = share_in(h0s, g0s, pre0s, w_out, 0, owners0, fr)

        out1 = scatter(out1.reshape(2, 2, 2, fr, d), [ZH, Y, X], OUT_ROUTES)
        in1 = in1.reshape(2, 2, 2, 2, 2, dr, 8 * fr)
        in1 = scatter(in1, [ZH, None, Y, X], IN_ROUTES)
        in1 = spread(spread(in1, 0, ZL), 1, CORE)
        in1 = in1.reshape(2, 2, dr, 2, 2, 2, fr)
        in1 = in1.transpose(2, 3, 0, 4, 5, 1, 6).reshape(dr, ff)

        out0 = line_reduce(out0.reshape(4, fr, d))
        in0 = line_reduce(in0.reshape(4, 8 * dr, 4 * fr))
        in0 = in0.reshape(2, 2, 2, dr, 4 * fr)
        in0 = spread(spread(spread(in0, 0, Y), 1, X), 2, CORE)
        in0 = in0.reshape(8, dr, 4, fr).transpose(1, 2, 0, 3).reshape(dr, ff)
        return jnp.stack([in0, in1]), jnp.stack([out0, out1])

    tok_spec = P("data", None)
    grad_spec = P(None, "data", None)
    return jax.shard_map(local_grads, mesh=mesh, in_specs=(tok_spec, tok_spec, P(), P()), out_specs=(grad_spec, grad_spec), check_vma=False)
```

```python
import jax
import jax.numpy as jnp
from jax import lax
from jax.experimental import pallas as pl
from jax.experimental.pallas import tpu as pltpu
from jax.sharding import PartitionSpec as P


CORE, X, Y, ZL, ZH = 1, 2, 4, 8, 16
F32, BF16 = jnp.float32, jnp.bfloat16


OUT_ROUTES = {"a": (4, (2, 4, 16)), "b": (3, (4, 2, 16)), "c": (3, (16, 2, 4))}
IN_ROUTES = {"a": (5, (4, 2, 16)), "b": (5, (2, 4, 16))}


def gelu_act(pre_f32):
    return jax.nn.gelu(pre_f32, approximate=True)


def dot(a, b, dims):
    return lax.dot_general(a, b, (dims, ((), ())), preferred_element_type=F32)


NN, NT, TN = ((1,), (0,)), ((1,), (1,)), ((0,), (0,))
ANY = pl.BlockSpec(memory_space=pl.ANY)
WHOLE = pl.BlockSpec(memory_space=pltpu.VMEM)


def grad_pre_of(pre, grad_act):
    _, pullback = jax.vjp(gelu_act, pre.astype(F32))
    return pullback(grad_act.astype(F32))[0].astype(BF16)


def start_rows(*streams, piece):
    todo = [[(ref, r, buf, sems) for ref in refs for r in range(0, ref.shape[0], piece)] for refs, buf, sems in streams]
    for k in range(len(todo[0])):
        for stream in todo:
            ref, r, buf, sems = stream[k]
            pltpu.make_async_copy(ref.at[pl.ds(r, piece)], buf.at[pl.ds(k * piece, piece)], sems.at[k]).start()


def wait_rows(buf, sems, piece, tile, i):
    for j in range(tile // piece):
        k = i * (tile // piece) + j
        view = buf.at[pl.ds(k * piece, piece)]
        pltpu.make_async_copy(view, view, sems.at[k]).wait()


def call(kernel, operands, in_specs, out_shape, out_specs, scratch, flops):
    nbytes = sum(o.size * o.dtype.itemsize for o in operands)
    return pl.pallas_call(
        kernel, out_shape=out_shape, in_specs=in_specs, out_specs=out_specs, scratch_shapes=scratch,
        compiler_params=pltpu.CompilerParams(vmem_limit_bytes=63 * 1024 * 1024),
        cost_estimate=pl.CostEstimate(flops=flops, bytes_accessed=nbytes, transcendentals=0),
    )(*operands)


def accumulate(i, steps, n_parts, chunk, part_of, acc, out_ref, out_sems):
    def part(c, _):
        at = pl.ds(pl.multiple_of(c * chunk, chunk), chunk)
        val = part_of(at)

        @pl.when(i == 0)
        def _():
            acc[at, :] = val

        @pl.when(i > 0)
        def _():
            acc[at, :] += val

        @pl.when(i == steps - 1)
        def _():
            pltpu.make_async_copy(acc.at[at], out_ref.at[at], out_sems.at[c]).start()

        return 0

    lax.fori_loop(0, n_parts, part, 0)


def finish(n_parts, chunk, acc, out_ref, out_sems):
    for c in range(n_parts):
        at = pl.ds(c * chunk, chunk)
        pltpu.make_async_copy(acc.at[at], out_ref.at[at], out_sems.at[c]).wait()


def sizes_of(blocks):
    piece = min(b.shape[0] for b in blocks)
    total = sum(b.shape[0] for b in blocks)
    return piece, total, blocks[0].shape[1]


def share_forward(blocks, w_in, layer, owners_of, fr):
    piece, total, d = sizes_of(blocks)
    piece = min(piece, 512)
    ff = w_in.shape[2]
    count = len(owners_of(jnp.int32(0)))
    cols, wide = count * fr, min(256, ff)
    nb, steps = len(blocks), total // piece

    def kernel(*refs):
        h_refs, (w_ref, pre_ref, act_ref, h_buf, win, w_buf, pre_buf, act_buf, sems, w_sems, out_sems) = refs[:nb], refs[nb:]
        owners = owners_of(lax.axis_index("data"))
        starts = [jnp.minimum((o * fr) // 128 * 128, ff - wide) for o in owners]
        for k, at in enumerate(starts):
            pltpu.make_async_copy(w_ref.at[layer, :, pl.ds(pl.multiple_of(at, 128), wide)], win.at[k], w_sems.at[k]).start()
        start_rows((h_refs, h_buf, sems), piece=piece)
        row = lax.broadcasted_iota(jnp.int32, (wide, fr), 0)
        col = lax.broadcasted_iota(jnp.int32, (wide, fr), 1)
        for k, (o, at) in enumerate(zip(owners, starts)):
            pltpu.make_async_copy(win.at[k], win.at[k], w_sems.at[k]).wait()
            pick = jnp.where(row == col + (o * fr - at), 1.0, 0.0).astype(BF16)
            w_buf[:, k * fr:(k + 1) * fr] = dot(win[k], pick, NN).astype(BF16)

        def outs(i, slot):
            rows = pl.ds(i * piece, piece)
            return (pltpu.make_async_copy(pre_buf.at[slot], pre_ref.at[rows], out_sems.at[slot, 0]),
                    pltpu.make_async_copy(act_buf.at[slot], act_ref.at[rows], out_sems.at[slot, 1]))

        def step(i, _):
            slot = i % 2
            wait_rows(h_buf, sems, piece, piece, i)

            @pl.when(i >= 2)
            def _():
                for c in outs(i - 2, slot):
                    c.wait()

            pre = dot(h_buf[pl.ds(i * piece, piece), :], w_buf[...], NN).astype(BF16)
            pre_buf[slot] = pre
            act_buf[slot] = gelu_act(pre.astype(F32)).astype(BF16)
            for c in outs(i, slot):
                c.start()
            return 0

        lax.fori_loop(0, steps, step, 0)
        for i in range(max(steps - 2, 0), steps):
            for c in outs(i, i % 2):
                c.wait()

    shape = jax.ShapeDtypeStruct((total, cols), BF16)
    return call(kernel, [*blocks, w_in], [ANY] * (nb + 1), [shape, shape], [ANY, ANY],
                [pltpu.VMEM((total, d), BF16), pltpu.VMEM((count, d, wide), BF16), pltpu.VMEM((d, cols), BF16),
                 pltpu.VMEM((2, piece, cols), BF16), pltpu.VMEM((2, piece, cols), BF16),
                 pltpu.SemaphoreType.DMA((steps,)), pltpu.SemaphoreType.DMA((count,)), pltpu.SemaphoreType.DMA((2, 2))],
                2 * total * d * cols)


def share_out(act, blocks):
    piece, total, d = sizes_of(blocks)
    piece = min(piece, 512)
    cols = act.shape[1]
    nb, tile = len(blocks), 2 * piece
    steps = total // tile
    n_parts = 5 if cols % 640 == 0 else 1
    chunk = cols // n_parts

    def kernel(*refs):
        act_ref, g_refs, (out_ref, act_buf, g_buf, acc, act_sems, sems, out_sems) = refs[0], refs[1:1 + nb], refs[1 + nb:]
        start_rows(([act_ref], act_buf, act_sems), (g_refs, g_buf, sems), piece=piece)

        def step(i, _):
            wait_rows(act_buf, act_sems, piece, tile, i)
            wait_rows(g_buf, sems, piece, tile, i)
            rows = pl.ds(i * tile, tile)
            accumulate(i, steps, n_parts, chunk, lambda at: dot(act_buf[rows, at], g_buf[rows, :], TN), acc, out_ref, out_sems)
            return 0

        lax.fori_loop(0, steps, step, 0)
        finish(n_parts, chunk, acc, out_ref, out_sems)

    return call(kernel, [act, *blocks], [ANY] * (nb + 1), jax.ShapeDtypeStruct((cols, d), F32), ANY,
                [pltpu.VMEM((total, cols), BF16), pltpu.VMEM((total, d), BF16), pltpu.VMEM((cols, d), F32),
                 pltpu.SemaphoreType.DMA((total // piece,)), pltpu.SemaphoreType.DMA((total // piece,)),
                 pltpu.SemaphoreType.DMA((n_parts,))],
                2 * total * d * cols)


def share_in(hs, gs, pre, w_out, layer, owners_of, fr):
    piece, total, d = sizes_of(hs)
    piece = min(piece, 512)
    cols = pre.shape[1]
    count = cols // fr
    nb, tile = len(hs), 2 * piece
    steps = total // tile
    n_parts = 5 if d % 640 == 0 else 1
    chunk = d // n_parts

    def kernel(*refs):
        h_refs, g_refs = refs[:nb], refs[nb:2 * nb]
        (pre_ref, w_ref, out_ref, h_buf, g_buf, pre_buf, v_buf, w_buf, acc,
         h_sems, g_sems, pre_sems, w_sems, out_sems) = refs[2 * nb:]
        copies = [pltpu.make_async_copy(w_ref.at[layer, pl.ds(pl.multiple_of(o * fr, fr), fr)],
                                        w_buf.at[pl.ds(k * fr, fr)], w_sems.at[k])
                  for k, o in enumerate(owners_of(lax.axis_index("data")))]
        for c in copies:
            c.start()

        def fetch(i, slot):
            return pltpu.make_async_copy(pre_ref.at[pl.ds(i * tile, tile)], pre_buf.at[slot], pre_sems.at[slot])

        fetch(0, 0).start()
        start_rows((g_refs, g_buf, g_sems), (h_refs, h_buf, h_sems), piece=piece)
        for c in copies:
            c.wait()

        def step(i, _):
            slot = i % 2
            wait_rows(g_buf, g_sems, piece, tile, i)
            fetch(i, slot).wait()

            @pl.when(i + 1 < steps)
            def _():
                fetch(i + 1, 1 - slot).start()

            def head(j, _):
                sub = pl.ds(j * piece, piece)
                e = dot(g_buf[pl.ds(i * tile + j * piece, piece), :], w_buf[...], NT).astype(BF16)
                v_buf[sub, :] = grad_pre_of(pre_buf[slot, sub, :], e)
                return 0

            lax.fori_loop(0, 2, head, 0)
            wait_rows(h_buf, h_sems, piece, tile, i)
            rows = pl.ds(i * tile, tile)
            accumulate(i, steps, n_parts, chunk, lambda at: dot(h_buf[rows, at], v_buf[...], TN), acc, out_ref, out_sems)
            return 0

        lax.fori_loop(0, steps, step, 0)
        finish(n_parts, chunk, acc, out_ref, out_sems)

    n_sem = total // piece
    return call(kernel, [*hs, *gs, pre, w_out], [ANY] * (2 * nb + 2), jax.ShapeDtypeStruct((d, cols), F32), ANY,
                [pltpu.VMEM((total, d), BF16), pltpu.VMEM((total, d), BF16), pltpu.VMEM((2, tile, cols), BF16),
                 pltpu.VMEM((tile, cols), BF16), pltpu.VMEM((cols, d), BF16), pltpu.VMEM((d, cols), F32),
                 pltpu.SemaphoreType.DMA((n_sem,)), pltpu.SemaphoreType.DMA((n_sem,)),
                 pltpu.SemaphoreType.DMA((2,)), pltpu.SemaphoreType.DMA((count,)), pltpu.SemaphoreType.DMA((n_parts,))],
                4 * total * d * cols)


def solution(mesh):
    n = mesh.shape["data"]

    def permute(v, pairs):
        return lax.ppermute(v, "data", pairs)

    def swap(v, bit):
        return permute(v, [(i, i ^ bit) for i in range(n)])

    def local_grads(tokens, targets, w_in, w_out):
        rows, d = tokens.shape
        ff = w_in.shape[2]
        dr, fr = d // n, ff // n
        scale = (rows * n) ** -0.5
        idx = lax.axis_index("data")

        def bit(b):
            return (idx // b) % 2

        z = idx // 8

        def plane_gather(v):
            vx, vy = swap(v, X), swap(v, Y)
            half = rows // 2
            lo = swap(vx[:half], Y)
            hi = swap(vy[half:], X)
            mine = [v, vx, vy, lo, hi]
            return mine + [swap(m, CORE) for m in mine]

        def pair_gather(v):
            mine = [v, swap(v, ZL)]
            return mine + [swap(m, CORE) for m in mine]

        def halve(arr, axis, b):
            keep = lax.dynamic_index_in_dim(arr, bit(b), axis, keepdims=False)
            send = lax.dynamic_index_in_dim(arr, 1 - bit(b), axis, keepdims=False)
            return keep + swap(send, b)

        def line_reduce(arr):
            right = [[(i, i + 8) for i in range(n) if i // 8 <= min(s, 2)] for s in range(3)]
            left = [[(i, i - 8) for i in range(n) if 3 - i // 8 <= min(s, 2)] for s in range(3)]

            def chunk(k):
                return lax.dynamic_index_in_dim(arr, jnp.clip(k, 0, 3), 0, keepdims=False)

            mine = lax.optimization_barrier([chunk(3 - s + z) for s in range(3)] + [chunk(s + z - 3) for s in range(3)] + [chunk(z)])
            recv_r = recv_l = None
            for s in range(3):
                send_r, send_l = mine[s], mine[3 + s]
                if s:
                    send_r, send_l = send_r + recv_r, send_l + recv_l
                recv_r = permute(send_r, right[s])
                recv_l = permute(send_l, left[s])
            return mine[6] + recv_r + recv_l

        def spread(arr, axis, b):
            keep = lax.dynamic_index_in_dim(arr, bit(b), axis, keepdims=False)
            send = lax.dynamic_index_in_dim(arr, 1 - bit(b), axis, keepdims=False)
            recv = swap(send, b)
            first = jnp.where(bit(b) == 0, keep, recv)
            second = jnp.where(bit(b) == 0, recv, keep)
            return jnp.stack([first, second], axis=axis)

        def scatter(arr, names, routes):
            width, at, parts = arr.shape[-1], 0, []
            for (tenths, order) in routes.values():
                size = width * tenths // 10
                part, left = lax.slice_in_dim(arr, at, at + size, axis=arr.ndim - 1), list(names)
                for b in order:
                    part = halve(part, left.index(b), b)
                    left.remove(b)
                parts.append(part)
                at += size
            return jnp.concatenate(parts, axis=-1)

        def owners1(i):
            return [zh * 16 + y * 4 + x * 2 + (i // ZL) % 2 * 8 + i % 2 for zh in range(2) for y in range(2) for x in range(2)]

        def owners0(i):
            return [zz * 8 + i % 8 for zz in range(4)]

        h0s = plane_gather(tokens)
        pre0 = dot(tokens, w_in[0], NN).astype(BF16)
        act0 = gelu_act(pre0.astype(F32)).astype(BF16)
        h1 = (tokens.astype(F32) + dot(act0, w_out[0], NN)).astype(BF16)
        h1s = pair_gather(h1)
        pre1 = dot(h1, w_in[1], NN).astype(BF16)
        act1 = gelu_act(pre1.astype(F32)).astype(BF16)
        h2 = (h1.astype(F32) + dot(act1, w_out[1], NN)).astype(BF16)
        g1 = ((h2.astype(F32) - targets.astype(F32)) * scale).astype(BF16)
        g1s = pair_gather(g1)
        grad_act1 = dot(g1, w_out[1], NT).astype(BF16)
        grad_pre1 = grad_pre_of(pre1, grad_act1)
        g0 = (g1.astype(F32) + dot(grad_pre1, w_in[1], NT)).astype(BF16)
        g0s = plane_gather(g0)

        pre1s, act1s = share_forward(h1s, w_in, 1, owners1, fr)
        pre0s, act0s = share_forward(h0s, w_in, 0, owners0, fr)
        out1 = share_out(act1s, g1s)
        in1 = share_in(h1s, g1s, pre1s, w_out, 1, owners1, fr)
        out0 = share_out(act0s, g0s)
        in0 = share_in(h0s, g0s, pre0s, w_out, 0, owners0, fr)

        out1 = scatter(out1.reshape(2, 2, 2, fr, d), [ZH, Y, X], OUT_ROUTES)
        in1 = in1.reshape(2, 2, 2, 2, 2, dr, 8 * fr)
        in1 = scatter(in1, [ZH, None, Y, X], IN_ROUTES)
        in1 = spread(spread(in1, 0, ZL), 1, CORE)
        in1 = in1.reshape(2, 2, dr, 2, 2, 2, fr)
        in1 = in1.transpose(2, 3, 0, 4, 5, 1, 6).reshape(dr, ff)

        out0 = line_reduce(out0.reshape(4, fr, d))
        in0 = line_reduce(in0.reshape(4, 8 * dr, 4 * fr))
        in0 = in0.reshape(2, 2, 2, dr, 4 * fr)
        in0 = spread(spread(spread(in0, 0, Y), 1, X), 2, CORE)
        in0 = in0.reshape(8, dr, 4, fr).transpose(1, 2, 0, 3).reshape(dr, ff)
        return jnp.stack([in0, in1]), jnp.stack([out0, out1])

    tok_spec = P("data", None)
    grad_spec = P(None, "data", None)
    return jax.shard_map(local_grads, mesh=mesh, in_specs=(tok_spec, tok_spec, P(), P()), out_specs=(grad_spec, grad_spec), check_vma=False)
```
